512 devices in a mesh: row: 64 (over y, z), col: 8 (over x, core).
Axes of the slice: x: 4, y: 4, z: 16, core: 2. Of those that a mesh axis runs over, the one named last changes fastest.
Arguments:
- kernel: float32 [16384, 16384], P('row', 'col')
- targets: float32 [16384, 64], P('row'), may hold values from -60 to 60
Outputs:
- schur: float32 [16384, 16384], P('row', 'col')
- factor: float32 [16384, 512], P('row')
- solved: float32 [16384, 64], P('row')
The draws below stay inside these ranges and needn't reach their ends.
All inputs are finite; a program needn't handle non-finite values.
Results may differ from the reference program's by a relative error of at most 0.00022.
Values sent between devices are 32-bit elements; how exact they have to be, the bound alone decides.
No kernel may reach another device: no remote copies, remote signals or barrier semaphores. Data moves between devices by JAX's collectives and lax.ppermute only.
A program may use at most 64 MiB of HBM per device.

```python
import jax
import jax.numpy as jnp
from jax import lax

NB = 256
RHS = 64
PANELS = 2
N = 16384
CB = 8


centre_dims = 24


ridge_rate = 0.001


def draw_kernel(key, part):
    first = jax.random.fold_in(key, 11)
    centres = jax.random.normal(first, (N, centre_dims), jnp.float32)
    centres = centres - jnp.mean(centres, axis=0)[None, :]
    spacing = 2.0 * jnp.sum(jnp.mean(centres * centres, axis=0))
    norms = jnp.sum(centres * centres, axis=1)
    gram = jnp.dot(centres, centres.T, precision=lax.Precision.HIGHEST)
    distance = jnp.maximum(norms[:, None] + norms[None, :] - 2.0 * gram, jnp.float32(0.0))
    matrix = jnp.exp(-distance / (2.0 * spacing))
    matrix = (matrix + matrix.T) * 0.5
    on_diag = jnp.arange(N)[:, None] == jnp.arange(N)[None, :]
    matrix = jnp.where(on_diag, jnp.float32(1.0 + ridge_rate * N), matrix)
    grid_cols = N // (NB * CB)
    return matrix.reshape(N, CB, grid_cols, NB).transpose(0, 2, 1, 3).reshape(N, N)


def block_levels(own_key, dims, split, least, top_value):
    gain, own = 1.0, jax.random.fold_in(own_key, 6)
    for position, parts in split:
        steps = jnp.exp(jax.random.uniform(jax.random.fold_in(own, position), (parts,), jnp.float32, least / len(split), top_value / len(split)))
        gain = gain * jnp.repeat(steps, dims[position] // parts).reshape([-1 if axis == position else 1 for axis in range(len(dims))])
    return gain


def centred(rng, extent, deviation, limit, shards=(), kind=jnp.bfloat16):
    entries = jax.random.normal(rng, extent, jnp.float32) * deviation
    if len(shards) > 0:
        entries = block_levels(rng, extent, shards, -0.22, 0.18) * entries
    return jnp.clip(entries, min=-limit, max=limit).astype(kind)


def setup_inputs(seed: int = 0) -> dict:
    key_list = jax.random.split(jax.random.key(seed), 3)
    return {
        "kernel": draw_kernel(jax.random.fold_in(key_list[2], 71), 0),
        "targets": centred(key_list[1], (N, RHS), 10.0, 60.0, ((0, 64),), jnp.float32),
    }


def reference(kernel, targets):
    grid_cols = N // (NB * CB)
    matrix = kernel.reshape(N, grid_cols, CB, NB).transpose(0, 2, 1, 3).reshape(N, N)
    rhs_now = targets
    block_ids = jnp.arange(N, dtype=jnp.int32) // NB
    columns_out = []
    for step in range(PANELS):
        start = step * NB
        lower = jnp.linalg.cholesky(matrix[start:start + NB, start:start + NB])
        column = matrix[:, start:start + NB]
        panel = lax.linalg.triangular_solve(lower, column, left_side=False, lower=True, transpose_a=True)
        panel = jnp.where((block_ids > step)[:, None], panel, jnp.float32(0.0))
        top = lax.linalg.triangular_solve(lower, rhs_now[start:start + NB], left_side=True, lower=True)
        rhs_now = rhs_now - jnp.dot(panel, top, precision=lax.Precision.HIGHEST)
        rhs_now = rhs_now.at[start:start + NB].set(top)
        columns_out.append(panel.at[start:start + NB].set(lower))
        row_blocks = matrix.reshape(N // NB, NB, N)
        panel_blocks = panel.reshape(N // NB, NB, NB)

        def update(pair):
            return pair[0] - jnp.dot(pair[1], panel.T, precision=lax.Precision.HIGHEST)
        matrix = lax.map(update, (row_blocks, panel_blocks)).reshape(N, N)
    schur = matrix.reshape(N, CB, grid_cols, NB).transpose(0, 2, 1, 3).reshape(N, N)
    return (schur, jnp.concatenate(columns_out, axis=1), rhs_now)
```

```python
import functools
import jax, jax.numpy as jnp
from jax import lax
from jax.sharding import Mesh
from jax.sharding import PartitionSpec as P
from jax.experimental import pallas as pl
from jax.experimental.pallas import tpu as pltpu
HI = lax.Precision.HIGHEST
NT = (((1,), (1,)), ((), ()))
NN = (((1,), (0,)), ((), ()))

def dot(a, b, dims):
    return lax.dot_general(a, b, dims, precision=HI, preferred_element_type=jnp.float32)

def inverse_factor(load, store):
    lane = lax.broadcasted_iota(jnp.int32, (8, 128), 1)
    sub = lax.broadcasted_iota(jnp.int32, (8, 128), 0)
    rows = [load(v) for v in range(16)]
    for b in range(16):
        first = 8 * b
        inside = (lane >= first) & (lane < first + 8)
        eye = jnp.where(lane == sub + first, 1.0, 0.0)
        piv = [jnp.broadcast_to(rows[b][:, first + j:first + j + 1], (8, 128)) for j in range(8)]
        head = jnp.where(inside, eye, rows[b])
        scale = jnp.zeros((8, 128), jnp.float32)
        recips, tops, heads = [], [], []
        for j in range(8):
            p = jnp.broadcast_to(piv[j][j:j + 1, :], (8, 128))
            recip = 1.0 / p
            scale = jnp.where(sub == j, lax.rsqrt(p), scale)
            top = {i: jnp.broadcast_to(piv[i][j:j + 1, :], (8, 128)) for i in range(j + 1, 8)}
            row = jnp.broadcast_to(head[j:j + 1, :], (8, 128))
            recips.append(recip); tops.append(top); heads.append(row)
            if j < 7:
                m = jnp.where(sub > j, piv[j] * recip, 0.0)
                for i in range(j + 1, 8):
                    piv[i] = piv[i] - m * top[i]
                head = head - m * row
        store(b, jnp.where(lane <= sub + first, head, 0.0) * scale)
        for v in range(b + 1, 16):
            cols = [jnp.broadcast_to(rows[v][:, first + j:first + j + 1], (8, 128)) for j in range(8)]
            rest = jnp.where(inside, 0.0, rows[v])
            for j in range(8):
                m = cols[j] * recips[j]
                for i in range(j + 1, 8):
                    cols[i] = cols[i] - m * tops[j][i]
                rest = rest - m * heads[j]
            rows[v] = rest

def factor_kernel(where_ref, d_ref, a_ref, b_ref, factor_ref, solved_ref, mid_ref, g_ref, work, low, inv, rhs):
    r = where_ref[0]
    for t in range(4):
        if t < 2:
            work[t, 0:256, :] = d_ref[:, 128 * t:128 * t + 128]
            work[t, 256:512, :] = d_ref[:, 256 + 128 * t:256 + 128 * t + 128]
        else:
            work[t, 0:256, :] = jnp.zeros((256, 128), jnp.float32)
            work[t, 256:512, :] = d_ref[:, 256 + 128 * t:256 + 128 * t + 128]
        work[t, 512:768, :] = a_ref[:, 128 * t:128 * t + 128]
    rhs[0:256, :] = d_ref[:, 768:832]
    rhs[256:512, :] = d_ref[:, 832:896]
    rhs[512:768, :] = b_ref[...]

    def step(t, carry):
        base = pl.multiple_of(t * 128, 128)
        def load(v):
            return work[t, pl.ds(base + 8 * v, 8), :]
        def store(v, x):
            inv[t, 8 * v:8 * v + 8, :] = x
        inverse_factor(load, store)
        w = inv[t]
        x = dot(work[t], w, NT)
        row = lax.broadcasted_iota(jnp.int32, (768, 128), 0)
        x = jnp.where(row >= base, x, 0.0)
        low[t] = x
        y = dot(w, rhs[pl.ds(base, 128), :], NN)
        rhs[pl.ds(base, 128), :] = y
        below = jnp.where(row >= base + 128, x, 0.0)
        rhs[...] = rhs[...] - dot(below, y, NN)
        for s in range(1, 4):
            @pl.when(t < s)
            def _():
                work[s] = work[s] - dot(x, low[t, 128 * s:128 * s + 128, :], NT)
        @pl.when(t == 1)
        def _():
            mid_ref[:, 0:128] = work[2, 512:768, :]
            mid_ref[:, 128:256] = work[3, 512:768, :]
        return carry
    lax.fori_loop(0, 4, step, 0)
    row = lax.broadcasted_iota(jnp.int32, (256, 128), 0)
    col = lax.broadcasted_iota(jnp.int32, (256, 128), 1)
    for t in range(4):
        block, off = t // 2, 128 * (t % 2)
        keep = (r > block) | ((r == block) & (row >= col + off))
        factor_ref[:, 128 * t:128 * t + 128] = jnp.where(keep, low[t, 512:768, :], 0.0)
    first, second = rhs[0:256, :], rhs[256:512, :]
    solved_ref[...] = jnp.where(r == 0, first, jnp.where(r == 1, second, rhs[512:768, :]))
    parts = [None] * 4
    for t in (3, 2, 1, 0):
        acc = jnp.where(r > t // 2, low[t, 512:768, :], 0.0)
        for s in range(t + 1, 4):
            acc = acc - dot(parts[s], low[t, 128 * s:128 * s + 128, :], NN)
        parts[t] = dot(acc, inv[t], NN)
        g_ref[:, 128 * t:128 * t + 128] = parts[t]

def factor_call(place, d, a, b):
    f32 = jnp.float32
    vm = pl.BlockSpec(memory_space=pltpu.VMEM)
    return pl.pallas_call(
        factor_kernel,
        out_shape=(jax.ShapeDtypeStruct((256, 512), f32), jax.ShapeDtypeStruct((256, 64), f32),
                   jax.ShapeDtypeStruct((256, 256), f32), jax.ShapeDtypeStruct((256, 512), f32)),
        in_specs=[pl.BlockSpec(memory_space=pltpu.SMEM), vm, vm, vm],
        out_specs=(vm, vm, vm, vm),
        scratch_shapes=[pltpu.VMEM((4, 768, 128), f32), pltpu.VMEM((4, 768, 128), f32),
                        pltpu.VMEM((4, 128, 128), f32), pltpu.VMEM((768, 64), f32)],
    )(place, d, a, b)


def update_kernel(place_ref, a_ref, g_ref, mid_ref, own_ref, up_ref, down_ref, far_ref, out_ref):
    r, y, c = place_ref[0], place_ref[1], place_ref[2]
    for step, chunk in ((0, own_ref), (1, up_ref), (3, down_ref), (2, far_ref)):
        start = pl.multiple_of(lax.rem(y + step, 4) * 512, 512)
        cols = pl.ds(start, 512)
        out_ref[:, cols] = a_ref[:, cols] - dot(g_ref[...], chunk[...], NT)

    @pl.when(c == 0)
    def _():
        out_ref[:, 0:256] = a_ref[:, 0:256]

    @pl.when((c == 1) & (r > 0))
    def _():
        out_ref[:, 0:256] = mid_ref[...]


def update_call(place, a, g, mid, chunks):
    vm = pl.BlockSpec(memory_space=pltpu.VMEM)
    return pl.pallas_call(
        update_kernel,
        out_shape=jax.ShapeDtypeStruct(a.shape, jnp.float32),
        in_specs=[pl.BlockSpec(memory_space=pltpu.SMEM)] + [vm] * 7,
        out_specs=vm,
        cost_estimate=pl.CostEstimate(flops=2 * 256 * 2048 * 512, bytes_accessed=9 << 20, transcendentals=0),
    )(place, a, g, mid, *chunks)


AXES = ("y", "z", "x", "k")
YS, ZS, XS, KS = range(4), range(16), range(4), range(2)


def at(y, z, x, k):
    return ((y * 16 + z % 16) * 4 + x) * 2 + k


def send(value, pairs):
    return lax.ppermute(value, AXES, pairs)


def shards(kernel, targets):
    y, z, x, k = (lax.axis_index(name) for name in AXES)
    r, c = y * 16 + z, x * 2 + k
    mine = kernel[:, 0:256]
    held = jnp.where(x == 0, mine, 0.0)
    for far in (2, 1, 3):
        held = held + send(mine, [(at(a, b, 0, e), at(a, b, far, e)) for a in YS for b in ZS for e in KS])
    other = lax.ppermute(held, "k", [(0, 1), (1, 0)])
    left = jnp.where(k == 0, held, other)
    right = jnp.where(k == 0, other, held)
    rows = jnp.concatenate([left, right], axis=1)

    def cut(value):
        return lax.dynamic_slice_in_dim(value, c * 32, 32, 0)
    part = jnp.concatenate([cut(rows), cut(targets)], axis=1)
    swapped = send(part, [(at(0, b, a, e), at(0, 1 - b, a, e)) for b in (0, 1) for a in XS for e in KS])
    top = jnp.where(z == 0, part, swapped)
    low = jnp.where(z == 0, swapped, part)
    whole = jnp.concatenate([top[:, 0:256], low[:, 0:512], top[:, 512:576], low[:, 512:576]], axis=1)
    got = jnp.where((y == 0) & (z < 2), whole, 0.0)
    for far in (2, 1, 3):
        got = got + send(whole, [(at(0, b, a, e), at(far, b, a, e)) for b in (0, 1) for a in XS for e in KS])
    source = got
    for hops in (((1, 7), (0, 10)), ((1, 4), (0, 13))):
        got = got + send(source, [(at(b, s, a, e), at(b, t, a, e)) for s, t in hops for b in YS for a in XS for e in KS])
    source = got
    for hops in (((1, 2), (4, 5), (7, 8), (0, 15), (13, 12), (10, 9)), ((4, 3), (7, 6), (13, 14), (10, 11))):
        got = got + send(source, [(at(b, s, a, e), at(b, t, a, e)) for s, t in hops for b in YS for a in XS for e in KS])
    diag = lax.all_gather(got, ("x", "k")).reshape(256, 896)

    def quarter(value, index):
        return lax.dynamic_slice_in_dim(value, lax.rem(index, 4) * 64, 64, 0)
    sources = [(b, 8 * h + e, e // 2, e % 2) for b in YS for h in (0, 1) for e in range(8)]
    away = lax.rem(z + 16 - c, 16)
    near = jnp.where(lax.rem(away, 8) == 0, quarter(rows, z), 0.0)
    for d in (1, 2, 3):
        near = near + send(quarter(rows, z + d), [(at(b, s, a, e), at(b, s + d, a, e)) for b, s, a, e in sources])
    def jump(d):
        return send(near, [(at(b, s + q, a, e), at(b, s + q + d, a, e)) for b, s, a, e in sources for q in range(4)])
    plus, minus, across = jump(4), jump(-4), jump(8)
    side = away // 4
    def pick(values):
        return jnp.where(side == 0, values[0], jnp.where(side == 1, values[1], jnp.where(side == 2, values[2], values[3])))
    pair = jnp.stack([pick((near, plus, across, minus)), pick((across, minus, near, plus))])
    full = jnp.zeros((2, 4, 64, 512), jnp.float32)
    shifted = [pair] + [lax.ppermute(pair, "z", [(b, (b + s) % 16) for b in ZS]) for s in (1, 15, 2)]
    for piece, s in zip(shifted, (0, 3, 1, 2)):
        full = lax.dynamic_update_slice(full, piece[:, None], (0, lax.rem(z + s, 4), 0, 0))
    own = full.reshape(512, 512)
    down = lax.ppermute(own, "y", [(b, (b + 1) % 4) for b in YS])
    up = lax.ppermute(own, "y", [(b, (b + 3) % 4) for b in YS])
    far = jnp.concatenate([
        lax.ppermute(down[:256], "y", [(b, (b + 1) % 4) for b in YS]),
        lax.ppermute(up[256:], "y", [(b, (b + 3) % 4) for b in YS]),
    ])

    factor, solved, mid, g = factor_call(jnp.stack([r]).astype(jnp.int32), diag, rows, targets)
    place = jnp.stack([r, y, c]).astype(jnp.int32)
    schur = update_call(place, kernel, g, mid, (own, up, down, far))
    return schur, factor, solved


def solution(mesh):
    finer = Mesh(mesh.devices.reshape(4, 16, 4, 2), AXES)
    row, col = ("y", "z"), ("x", "k")
    return jax.shard_map(
        shards,
        mesh=finer,
        in_specs=(P(row, col), P(row, None)),
        out_specs=(P(row, col), P(row, None), P(row, None)),
        check_vma=False,
    )
```
